32 devices in a mesh: seq: 8 (over z, x), kvh: 4 (over y, core).
Axes of the slice: x: 2, y: 2, z: 4, core: 2. Of those that a mesh axis runs over, the one named last changes fastest.
Arguments:
- queries: bfloat16 [1024, 28, 128], P('seq', 'kvh'), may hold values from -80 to 80
- new_keys: bfloat16 [1024, 4, 128], P('seq', 'kvh'), may hold values from -8 to 8
- cache_keys: bfloat16 [512, 4, 128], P('seq', 'kvh'), may hold values from -1.1953125 to 1.1953125
- window_start: int32 [8], replicated, may hold values from 0 to 512, as said below
- owner_slot: int32 [8], replicated, may hold values from 0 to 511, as said below
Outputs:
- relevance: bfloat16 [1024, 28, 512], P('seq', 'kvh')
- rep_bank: bfloat16 [512, 4, 128], P('seq', 'kvh')
The draws below stay inside these ranges and needn't reach their ends.
Inputs may be any that keep to these rules, and one draw needn't show every extreme that they name: `window_start`: each window lies inside the new tokens; some window begins at the first new token and some ends at the last. `owner_slot`: the slots are distinct; the first and the last memory block are always among them.
All inputs are finite; a program needn't handle non-finite values.
Results may differ from the reference program's by a relative error of at most 0.0018.
Values may be sent and summed in bfloat16 or wider, within the bound.
A program may use at most 64 MiB of HBM per device.

```python
import math
import jax
import jax.numpy as jnp
from jax import lax

HEADS = 28
KVH = 4
HD = 128
BLK = 128
WIN = 512
QTOK = 1024
NEWB = 8
CACHEB = 512


def joint_draw(key):
    key_query = jax.random.fold_in(key, 11)
    key_keys = jax.random.fold_in(key, 12)
    key_window = jax.random.fold_in(key, 13)
    key_ends = jax.random.fold_in(key, 16)
    starts = jax.random.randint(key_window, (NEWB,), 0, QTOK - WIN + 1).astype(jnp.int32)
    end_keys = jax.random.split(key_ends, 2)
    first_pick = jax.random.randint(end_keys[0], (), 0, NEWB).astype(jnp.int32)
    second_pick = ((first_pick + 1 + jax.random.randint(end_keys[1], (), 0, NEWB - 1)) % NEWB).astype(jnp.int32)
    starts = starts.at[first_pick].set(jnp.int32(0))
    starts = starts.at[second_pick].set(jnp.int32(QTOK - WIN))
    key_rows = jnp.clip(jax.random.normal(key_keys, (QTOK, KVH, HD), jnp.float32), -8.0, 8.0)
    query_rows = jnp.clip(jax.random.normal(key_query, (QTOK, HEADS, HD), jnp.float32), -8.0, 8.0)
    return (query_rows, key_rows, starts)


def draw_queries(key, part):
    return joint_draw(key)[0].astype(jnp.bfloat16)


def draw_new_keys(key, part):
    return joint_draw(key)[1].astype(jnp.bfloat16)


def draw_window_start(key, part):
    return joint_draw(key)[2]


def draw_owner_slot(key, part):
    inner = jax.random.permutation(jax.random.fold_in(key, 21), CACHEB - 2)[:NEWB - 2].astype(jnp.int32) + 1
    ends = jnp.array([0, CACHEB - 1], dtype=jnp.int32)
    slots = jnp.concatenate([ends, inner])
    order = jax.random.permutation(jax.random.fold_in(key, 22), NEWB)
    return slots[order].astype(jnp.int32)


def block_scale(key, extent, cuts, low, largest):
    level, own = 1.0, jax.random.fold_in(key, 6)
    for position, shards_of in cuts:
        draws = jnp.exp(jax.random.uniform(jax.random.fold_in(own, position), (shards_of,), jnp.float32, low / len(cuts), largest / len(cuts)))
        level = level * jnp.repeat(draws, extent[position] // shards_of).reshape([-1 if axis == position else 1 for axis in range(len(extent))])
    return level


def normal_values(rng, shape, deviation, reach, pieces=(), held_as=jnp.bfloat16):
    level = block_scale(rng, shape, pieces, -0.22, 0.18) if pieces else 1.0
    values = jax.random.normal(rng, shape, jnp.float32) * deviation * level
    return jnp.minimum(jnp.maximum(values, -reach), reach).astype(held_as)


def setup_inputs(seed: int = 0) -> dict:
    key_list = jax.random.split(jax.random.key(seed), 6)
    queries = draw_queries(jax.random.fold_in(key_list[5], 71), 0)
    new_keys = draw_new_keys(jax.random.fold_in(key_list[5], 71), 0)
    cache_keys = normal_values(key_list[2], (CACHEB, KVH, HD), 0.15, 1.1953125, ((0, 8), (1, 4)))
    window_start = draw_window_start(jax.random.fold_in(key_list[5], 71), 0)
    owner_slot = draw_owner_slot(jax.random.fold_in(key_list[5], 71), 0)
    return {"queries": queries, "new_keys": new_keys, "cache_keys": cache_keys, "window_start": window_start, "owner_slot": owner_slot}


def reference(queries, new_keys, cache_keys, window_start, owner_slot):
    group_size = HEADS // KVH
    score_scale = 1.0 / math.sqrt(HD)

    def one_block(block_index):
        begin = window_start[block_index].astype(jnp.int32)
        window_q = lax.dynamic_slice_in_dim(queries, begin, WIN, 0).astype(jnp.float32)
        window_q = window_q.reshape(WIN, KVH, group_size, HD)
        block_keys = lax.dynamic_slice_in_dim(new_keys, (block_index * BLK).astype(jnp.int32), BLK, 0).astype(jnp.float32)
        scores = jnp.einsum('wgjd,kgd->wgjk', window_q, block_keys, precision=lax.Precision.HIGHEST) * score_scale
        softmax_weights = jax.nn.softmax(scores, axis=-1)
        weights = lax.optimization_barrier(jnp.sum(softmax_weights, axis=(0, 2))) / (group_size * WIN)
        merged = jnp.einsum('gk,kgd->gd', weights, block_keys, precision=lax.Precision.HIGHEST)
        return merged.astype(jnp.bfloat16)
    representative = lax.map(one_block, jnp.arange(NEWB, dtype=jnp.int32))
    key_bank = cache_keys.at[owner_slot].set(representative)
    query_block = math.gcd(QTOK, 512)
    bank_float = key_bank.astype(jnp.float32)

    def score_block(query_part):
        grouped = query_part.astype(jnp.float32).reshape(query_block, KVH, group_size, HD)
        result = jnp.einsum('tgjd,bgd->tgjb', grouped, bank_float) * score_scale
        return result.astype(jnp.bfloat16).reshape(query_block, HEADS, CACHEB)
    relevance = lax.map(score_block, queries.reshape(QTOK // query_block, query_block, HEADS, HD))
    return (relevance.reshape(QTOK, HEADS, CACHEB), key_bank)
```

```python
import functools
import math

import jax
import jax.numpy as jnp
from jax import lax
from jax.experimental import pallas as pl
from jax.experimental.pallas import tpu as pltpu
from jax.sharding import PartitionSpec as P

BLK = 128
WIN = 512
LOG2E = 1.4426950408889634
NT = (((1,), (1,)), ((), ()))


def each(count, body):
    if count <= 8:
        for i in range(count):
            body(i)
    else:
        lax.fori_loop(0, count, lambda i, c: (body(i), c)[1], 0)


def refresh_kernel(
    n, start_ref, slot_ref, q_hbm, k_hbm, c_hbm, rel_ref, bank_ref,
    q_v, q_t, keys, cache, mine, parts, bank,
    load_sem, ks_sem, kr_sem, cs_sem, cr_sem, ps_sem, pr_sem,
):
    group, toks, dim = q_v.shape
    ktoks = keys.shape[1]
    local = cache.shape[1]
    slots = n * local
    per = ktoks // BLK
    blocks = n * per
    rows = group * toks
    scale = 1.0 / math.sqrt(dim)
    me = lax.axis_index("seq")

    load_k = pltpu.make_async_copy(k_hbm, keys.at[me], load_sem.at[0])
    load_q = pltpu.make_async_copy(q_hbm, q_v, load_sem.at[1])
    load_c = pltpu.make_async_copy(c_hbm, cache.at[me], load_sem.at[2])
    load_k.start()
    load_q.start()
    load_c.start()

    barrier = pltpu.get_barrier_semaphore()

    def greet(i):
        peer = lax.rem(me + 1 + i, n)
        pl.semaphore_signal(
            barrier, inc=1, device_id={"seq": peer}, device_id_type=pl.DeviceIdType.MESH
        )

    each(n - 1, greet)

    def link(src, dst, s_sem, r_sem, peer):
        return pltpu.make_async_remote_copy(
            src_ref=src, dst_ref=dst, send_sem=s_sem, recv_sem=r_sem,
            device_id={"seq": peer}, device_id_type=pl.DeviceIdType.MESH,
        )

    def key_copy(slot, peer):
        return link(keys.at[slot], keys.at[slot], ks_sem.at[peer], kr_sem.at[slot], peer)

    def cache_copy(slot, peer):
        return link(cache.at[slot], cache.at[slot], cs_sem.at[peer], cr_sem.at[slot], peer)

    def part_copy(slot, peer, src):
        return link(src, parts.at[slot], ps_sem.at[peer], pr_sem.at[slot], peer)

    load_k.wait()
    pl.semaphore_wait(barrier, n - 1)
    each(n - 1, lambda i: key_copy(me, lax.rem(me + 1 + i, n)).start())
    load_c.wait()
    each(n - 1, lambda i: cache_copy(me, lax.rem(me + 1 + i, n)).start())

    load_q.wait()
    for j in range(group):
        q_t[:, j * toks:(j + 1) * toks] = q_v[j].T

    position = me * toks + lax.broadcasted_iota(jnp.int32, (1, toks), 1)

    def partial(owner):
        for p in range(per):
            index = owner * per + p
            kb = keys[owner, p * BLK:(p + 1) * BLK, :]
            begin = start_ref[index]
            mask = jnp.where((position >= begin) & (position < begin + WIN), 1.0, 0.0)
            s = jnp.dot(kb, q_t[...], preferred_element_type=jnp.float32)
            top = jnp.max(s, axis=0, keepdims=True)
            e = jnp.exp2((s - top) * (scale * LOG2E))
            total = jnp.sum(e, axis=0, keepdims=True)
            acc = None
            for j in range(group):
                cols = slice(j * toks, (j + 1) * toks)
                term = e[:, cols] * (mask / total[:, cols])
                acc = term if acc is None else acc + term
            weight = jnp.sum(acc, axis=1, keepdims=True)
            rep = jnp.sum(weight * kb.astype(jnp.float32), axis=0, keepdims=True)
            mine[pl.ds(index, 1), :] = rep

    partial(me)

    def arrive(i):
        owner = lax.rem(me + n - 1 - i, n)
        key_copy(owner, owner).wait_recv()
        partial(owner)

    each(n - 1, arrive)
    each(n - 1, lambda i: part_copy(me, lax.rem(me + 1 + i, n), mine).start())

    each(n - 1, lambda i: cache_copy(lax.rem(me + n - 1 - i, n), me).wait_recv())
    hits = jnp.where(
        lax.broadcasted_iota(jnp.int32, (slots, blocks), 0) == slot_ref[...], 1.0, 0.0
    )
    taken = jnp.max(hits, axis=1, keepdims=True)
    hits = hits.astype(jnp.bfloat16)
    old = cache[...].reshape(slots, dim)

    each(n - 1, lambda i: part_copy(lax.rem(me + n - 1 - i, n), me, mine).wait_recv())
    parts[me] = mine[...]
    if n <= 8:
        rep_sum = parts[0]
        for d in range(1, n):
            rep_sum = rep_sum + parts[d]
    else:
        rep_sum = lax.fori_loop(1, n, lambda d, c: c + parts[d], parts[0])
    rep = (rep_sum * (1.0 / (group * WIN))).astype(jnp.bfloat16)
    placed = jnp.dot(hits, rep, preferred_element_type=jnp.float32)
    bank[...] = jnp.where(taken > 0.5, placed, old.astype(jnp.float32)).astype(jnp.bfloat16)
    bank_ref[...] = bank[pl.ds(pl.multiple_of(me * local, local), local), :]

    def relate(j):
        r = lax.dot_general(q_v[j], bank[...], NT, preferred_element_type=jnp.float32)
        rel_ref[j] = (r * scale).astype(jnp.bfloat16)

    each(group, relate)

    def drain(i):
        peer = lax.rem(me + 1 + i, n)
        key_copy(me, peer).wait_send()
        cache_copy(me, peer).wait_send()
        part_copy(me, peer, mine).wait_send()

    each(n - 1, drain)


def per_device(n, queries, new_keys, cache_keys, window_start, owner_slot):
    toks, group, dim = queries.shape
    ktoks, local = new_keys.shape[0], cache_keys.shape[0]
    blocks = window_start.shape[0]
    slots = n * local
    any_spec = pl.BlockSpec(memory_space=pl.ANY)
    vmem_spec = pl.BlockSpec(memory_space=pltpu.VMEM)
    bf16 = jnp.bfloat16
    rel, bank = pl.pallas_call(
        functools.partial(refresh_kernel, n),
        out_shape=(
            pltpu.VMEM((group, toks, slots), bf16),
            pltpu.VMEM((local, dim), bf16),
        ),
        in_specs=[
            pl.BlockSpec(memory_space=pltpu.SMEM), vmem_spec, any_spec, any_spec, any_spec,
        ],
        out_specs=(vmem_spec, vmem_spec),
        scratch_shapes=[
            pltpu.VMEM((group, toks, dim), bf16),
            pltpu.VMEM((dim, group * toks), bf16),
            pltpu.VMEM((n, ktoks, dim), bf16),
            pltpu.VMEM((n, local, dim), bf16),
            pltpu.VMEM((blocks, dim), jnp.float32),
            pltpu.VMEM((n, blocks, dim), jnp.float32),
            pltpu.VMEM((slots, dim), bf16),
            pltpu.SemaphoreType.DMA((3,)),
        ] + [pltpu.SemaphoreType.DMA((n,))] * 6,
        compiler_params=pltpu.CompilerParams(
            collective_id=0, has_side_effects=True, vmem_limit_bytes=40 * 1024 * 1024
        ),
        name="refresh",
    )(
        window_start,
        owner_slot.reshape(1, blocks),
        jnp.transpose(queries, (1, 0, 2)),
        new_keys.reshape(ktoks, dim),
        cache_keys.reshape(local, dim),
    )
    return jnp.transpose(rel, (1, 0, 2)), bank[:, None, :]


def solution(mesh):
    spec = P("seq", "kvh", None)
    return jax.shard_map(
        functools.partial(per_device, mesh.shape["seq"]),
        mesh=mesh,
        in_specs=(spec, spec, spec, P(), P()),
        out_specs=(spec, spec),
        check_vma=False,
    )
```

```python
import functools
import math

import jax
import jax.numpy as jnp
from jax import lax
from jax.experimental import pallas as pl
from jax.experimental.pallas import tpu as pltpu
from jax.sharding import PartitionSpec as P

BLK = 128
WIN = 512
VMEM = 67043328
LOG2E = 1.4426950408889634
NT = (((1,), (1,)), ((), ()))


def each(count, body):
    if count <= 8:
        for i in range(count):
            body(i)
    else:
        lax.fori_loop(0, count, lambda i, c: (body(i), c)[1], 0)


def refresh_kernel(
    n, start_hbm, slot_hbm, q_hbm, k_hbm, c_hbm, rel_ref, bank_ref,
    start_ref, slot_ref, q_v, q_t, keys, cache, mine, parts, bank,
    load_sem, ks_sem, kr_sem, cs_sem, cr_sem, ps_sem, pr_sem,
):
    group, toks, dim = q_v.shape
    ktoks = keys.shape[1]
    local = cache.shape[1]
    slots = n * local
    per = ktoks // BLK
    blocks = n * per
    rows = group * toks
    scale = 1.0 / math.sqrt(dim)
    me = lax.axis_index("seq")

    load_k = pltpu.make_async_copy(k_hbm, keys.at[me], load_sem.at[0])
    load_q = pltpu.make_async_copy(q_hbm, q_v, load_sem.at[1])
    load_c = pltpu.make_async_copy(c_hbm, cache.at[me], load_sem.at[2])
    load_w = pltpu.make_async_copy(start_hbm, start_ref, load_sem.at[3])
    load_s = pltpu.make_async_copy(slot_hbm, slot_ref, load_sem.at[4])
    load_k.start()
    load_c.start()
    load_q.start()
    load_w.start()
    load_s.start()

    side = lax.rem(me, 2)
    row = lax.div(me, 2)
    height = n // 2
    partner = me + 1 - 2 * side
    above = row < height - 1
    below = row > 0

    def greet(peer):
        pl.semaphore_signal(
            barrier, inc=1, device_id={"seq": peer}, device_id_type=pl.DeviceIdType.MESH
        )

    barrier = pltpu.get_barrier_semaphore()
    greet(partner)
    pl.when(above)(lambda: greet(me + 2))
    pl.when(below)(lambda: greet(me - 2))

    def link(src, dst, s_sem, r_sem, peer):
        return pltpu.make_async_remote_copy(
            src_ref=src, dst_ref=dst, send_sem=s_sem, recv_sem=r_sem,
            device_id={"seq": peer}, device_id_type=pl.DeviceIdType.MESH,
        )

    def key_copy(slot, way, peer):
        return link(keys.at[slot], keys.at[slot], ks_sem.at[way, slot], kr_sem.at[slot], peer)

    def cache_copy(slot, way, peer):
        return link(cache.at[slot], cache.at[slot], cs_sem.at[way, slot], cr_sem.at[slot], peer)

    def part_copy(slot, peer, src):
        return link(src, parts.at[slot], ps_sem.at[peer], pr_sem.at[slot], peer)

    def chain(copy, act):
        def column(slot, up, down):
            if up:
                pl.when(above)(lambda: act(copy(slot, 0, me + 2)))
            if down:
                pl.when(below)(lambda: act(copy(slot, 1, me - 2)))
            act(copy(slot, 2, partner))
        return column

    send_key = chain(key_copy, lambda c: c.start())
    send_cache = chain(cache_copy, lambda c: c.start())

    load_k.wait()
    pl.semaphore_wait(
        barrier, 1 + jnp.where(above, 1, 0) + jnp.where(below, 1, 0)
    )
    send_key(me, True, True)
    load_c.wait()
    send_cache(me, True, True)

    load_q.wait()
    load_w.wait()
    load_s.wait()
    for j in range(group):
        q_t[:, j * toks:(j + 1) * toks] = q_v[j].T

    position = me * toks + lax.broadcasted_iota(jnp.int32, (1, toks), 1)

    def partial(owner):
        for p in range(per):
            index = owner * per + p
            kb = keys[owner, p * BLK:(p + 1) * BLK, :]
            begin = start_ref[index]
            mask = jnp.where((position >= begin) & (position < begin + WIN), 1.0, 0.0)
            s = jnp.dot(kb, q_t[...], preferred_element_type=jnp.float32)
            top = jnp.max(s, axis=0, keepdims=True)
            e = jnp.exp2((s - top) * (scale * LOG2E))
            total = jnp.sum(e, axis=0, keepdims=True)
            acc = None
            for j in range(group):
                cols = slice(j * toks, (j + 1) * toks)
                term = e[:, cols] * (mask / total[:, cols])
                acc = term if acc is None else acc + term
            weight = jnp.sum(acc, axis=1, keepdims=True)
            rep = jnp.sum(weight * kb.astype(jnp.float32), axis=0, keepdims=True)
            mine[pl.ds(index, 1), :] = rep

    partial(me)

    def visit(s, copy, send):
        def from_below():
            copy(me - 2 * (s + 1), 0, me).wait_recv()
            send(me - 2 * (s + 1), True, False)

        def from_above():
            copy(me + 2 * (s + 1), 1, me).wait_recv()
            send(me + 2 * (s + 1), False, True)

        pl.when(row - 1 - s >= 0)(from_below)
        pl.when(row + 1 + s < height)(from_above)

    def both(s, act, base):
        pl.when(row - s >= 0)(lambda: act(base - 2 * s))
        pl.when(row + s < height)(lambda: act(base + 2 * s))

    def take_key(slot):
        key_copy(slot, 2, me).wait_recv()
        partial(slot)

    def take_cache(slot):
        cache_copy(slot, 2, me).wait_recv()

    def key_step(s):
        visit(s, key_copy, send_key)
        if isinstance(s, int) and s == 0:
            take_key(partner)
        else:
            both(s, take_key, partner)
        both(s + 1, partial, me)
        visit(s, cache_copy, send_cache)

    key_step(0)
    if height <= 4:
        for s in range(1, height - 1):
            key_step(s)
    else:
        lax.fori_loop(1, height - 1, lambda s, c: (key_step(s), c)[1], 0)
    both(height - 1, take_key, partner)

    each(n - 1, lambda i: part_copy(me, lax.rem(me + 1 + i, n), mine).start())

    take_cache(partner)
    if height <= 4:
        for s in range(1, height):
            both(s, take_cache, partner)
    else:
        lax.fori_loop(1, height, lambda s, c: (both(s, take_cache, partner), c)[1], 0)
    hits = jnp.where(
        lax.broadcasted_iota(jnp.int32, (slots, blocks), 0) == slot_ref[...], 1.0, 0.0
    )
    taken = jnp.max(hits, axis=1, keepdims=True)
    hits = hits.astype(jnp.bfloat16)
    old = cache[...].reshape(slots, dim)

    each(n - 1, lambda i: part_copy(lax.rem(me + n - 1 - i, n), me, mine).wait_recv())
    parts[me] = mine[...]
    if n <= 8:
        rep_sum = parts[0]
        for d in range(1, n):
            rep_sum = rep_sum + parts[d]
    else:
        rep_sum = lax.fori_loop(1, n, lambda d, c: c + parts[d], parts[0])
    rep = (rep_sum * (1.0 / (group * WIN))).astype(jnp.bfloat16)
    placed = jnp.dot(hits, rep, preferred_element_type=jnp.float32)
    bank[...] = jnp.where(taken > 0.5, placed, old.astype(jnp.float32)).astype(jnp.bfloat16)
    bank_ref[...] = bank[pl.ds(pl.multiple_of(me * local, local), local), :]

    def relate(j):
        r = lax.dot_general(q_v[j], bank[...], NT, preferred_element_type=jnp.float32)
        rel_ref[j] = (r * scale).astype(jnp.bfloat16)

    each(group, relate)

    def drain(i):
        part_copy(me, lax.rem(me + 1 + i, n), mine).wait_send()

    each(n - 1, drain)
    for copy in (key_copy, cache_copy):
        done = chain(copy, lambda c: c.wait_send())
        done(me, True, True)

        def finish(s, done=done):
            pl.when(row - s >= 0)(lambda: done(me - 2 * s, True, False))
            pl.when(row + s < height)(lambda: done(me + 2 * s, False, True))

        if height <= 4:
            for s in range(1, height):
                finish(s)
        else:
            lax.fori_loop(1, height, lambda s, c: (finish(s), c)[1], 0)


def per_device(n, queries, new_keys, cache_keys, window_start, owner_slot):
    toks, group, dim = queries.shape
    ktoks, local = new_keys.shape[0], cache_keys.shape[0]
    blocks = window_start.shape[0]
    slots = n * local
    hbm_spec = pl.BlockSpec(memory_space=pltpu.HBM)
    vmem_spec = pl.BlockSpec(memory_space=pltpu.VMEM)
    bf16 = jnp.bfloat16
    rel, bank = pl.pallas_call(
        functools.partial(refresh_kernel, n),
        out_shape=(
            pltpu.VMEM((group, toks, slots), bf16),
            pltpu.VMEM((local, dim), bf16),
        ),
        in_specs=[hbm_spec] * 5,
        out_specs=(vmem_spec, vmem_spec),
        scratch_shapes=[
            pltpu.SMEM((blocks,), jnp.int32),
            pltpu.VMEM((1, blocks), jnp.int32),
            pltpu.VMEM((group, toks, dim), bf16),
            pltpu.VMEM((dim, group * toks), bf16),
            pltpu.VMEM((n, ktoks, dim), bf16),
            pltpu.VMEM((n, local, dim), bf16),
            pltpu.VMEM((blocks, dim), jnp.float32),
            pltpu.VMEM((n, blocks, dim), jnp.float32),
            pltpu.VMEM((slots, dim), bf16),
            pltpu.SemaphoreType.DMA((5,)),
        ] + [pltpu.SemaphoreType.DMA((3, n)), pltpu.SemaphoreType.DMA((n,))] * 2
        + [pltpu.SemaphoreType.DMA((n,))] * 2,
        compiler_params=pltpu.CompilerParams(
            collective_id=0, has_side_effects=True, vmem_limit_bytes=VMEM - 2 * (group * toks * slots + local * dim) - 16384
        ),
        name="refresh",
    )(
        window_start,
        owner_slot.reshape(1, blocks),
        jnp.transpose(queries, (1, 0, 2)),
        new_keys.reshape(ktoks, dim),
        cache_keys.reshape(local, dim),
    )
    return jnp.transpose(rel, (1, 0, 2)), bank[:, None, :]


def solution(mesh):
    spec = P("seq", "kvh", None)
    return jax.shard_map(
        functools.partial(per_device, mesh.shape["seq"]),
        mesh=mesh,
        in_specs=(spec, spec, spec, P(), P()),
        out_specs=(spec, spec),
        check_vma=False,
    )
```

```python
import functools
import math

import jax
import jax.numpy as jnp
from jax import lax
from jax.experimental import pallas as pl
from jax.experimental.pallas import tpu as pltpu
from jax.sharding import PartitionSpec as P

BLK = 128
WIN = 512
VMEM = 67043328
LOG2E = 1.4426950408889634
NT = (((1,), (1,)), ((), ()))


def each(count, body):
    if count <= 8:
        for i in range(count):
            body(i)
    else:
        lax.fori_loop(0, count, lambda i, c: (body(i), c)[1], 0)


def refresh_kernel(
    n, start_hbm, slot_hbm, q_hbm, k_hbm, c_hbm, q_v, bank,
    start_ref, slot_ref, q_t, keys, cache, mine, parts,
    load_sem, ks_sem, kr_sem, cs_sem, cr_sem, ps_sem, pr_sem,
):
    group, toks, dim = q_v.shape
    ktoks = keys.shape[1]
    local = cache.shape[1]
    slots = n * local
    per = ktoks // BLK
    blocks = n * per
    rows = group * toks
    scale = 1.0 / math.sqrt(dim)
    me = lax.axis_index("seq")

    load_k = pltpu.make_async_copy(k_hbm, keys.at[me], load_sem.at[0])
    load_q = pltpu.make_async_copy(q_hbm, q_v, load_sem.at[1])
    load_c = pltpu.make_async_copy(c_hbm, cache.at[me], load_sem.at[2])
    load_w = pltpu.make_async_copy(start_hbm, start_ref, load_sem.at[3])
    load_s = pltpu.make_async_copy(slot_hbm, slot_ref, load_sem.at[4])
    load_k.start()
    load_c.start()
    load_q.start()
    load_w.start()
    load_s.start()

    barrier = pltpu.get_barrier_semaphore()

    def greet(i):
        peer = lax.rem(me + 1 + i, n)
        pl.semaphore_signal(
            barrier, inc=1, device_id={"seq": peer}, device_id_type=pl.DeviceIdType.MESH
        )

    each(n - 1, greet)

    def link(src, dst, s_sem, r_sem, peer):
        return pltpu.make_async_remote_copy(
            src_ref=src, dst_ref=dst, send_sem=s_sem, recv_sem=r_sem,
            device_id={"seq": peer}, device_id_type=pl.DeviceIdType.MESH,
        )

    def key_copy(slot, peer):
        return link(keys.at[slot], keys.at[slot], ks_sem.at[peer], kr_sem.at[slot], peer)

    def cache_copy(slot, peer):
        return link(cache.at[slot], cache.at[slot], cs_sem.at[peer], cr_sem.at[slot], peer)

    def part_copy(slot, peer, src):
        return link(src, parts.at[slot], ps_sem.at[peer], pr_sem.at[slot], peer)

    load_k.wait()
    pl.semaphore_wait(barrier, n - 1)
    each(n - 1, lambda i: key_copy(me, lax.rem(me + 1 + i, n)).start())
    load_c.wait()

    load_q.wait()
    load_w.wait()
    load_s.wait()
    for j in range(group):
        q_t[:, j * toks:(j + 1) * toks] = q_v[j].T

    position = me * toks + lax.broadcasted_iota(jnp.int32, (1, toks), 1)

    def partial(owner):
        for p in range(per):
            index = owner * per + p
            kb = keys[owner, p * BLK:(p + 1) * BLK, :]
            begin = start_ref[index]
            mask = jnp.where((position >= begin) & (position < begin + WIN), 1.0, 0.0)
            s = jnp.dot(kb, q_t[...], preferred_element_type=jnp.float32)
            top = jnp.max(s, axis=0, keepdims=True)
            e = jnp.exp2((s - top) * (scale * LOG2E))
            total = jnp.sum(e, axis=0, keepdims=True)
            acc = None
            for j in range(group):
                cols = slice(j * toks, (j + 1) * toks)
                term = e[:, cols] * (mask / total[:, cols])
                acc = term if acc is None else acc + term
            weight = jnp.sum(acc, axis=1, keepdims=True)
            rep = jnp.sum(weight * kb.astype(jnp.float32), axis=0, keepdims=True)
            mine[pl.ds(index, 1), :] = rep

    partial(me)

    def arrive(i):
        owner = lax.rem(me + n - 1 - i, n)
        key_copy(owner, owner).wait_recv()
        partial(owner)

    each(n - 1, arrive)
    each(n - 1, lambda i: part_copy(me, lax.rem(me + 1 + i, n), mine).start())
    each(n - 1, lambda i: cache_copy(me, lax.rem(me + 1 + i, n)).start())

    each(n - 1, lambda i: cache_copy(lax.rem(me + n - 1 - i, n), me).wait_recv())
    hits = jnp.where(
        lax.broadcasted_iota(jnp.int32, (slots, blocks), 0) == slot_ref[...], 1.0, 0.0
    )
    taken = jnp.max(hits, axis=1, keepdims=True)
    hits = hits.astype(jnp.bfloat16)
    old = cache[...].reshape(slots, dim)

    each(n - 1, lambda i: part_copy(lax.rem(me + n - 1 - i, n), me, mine).wait_recv())
    parts[me] = mine[...]
    if n <= 8:
        rep_sum = parts[0]
        for d in range(1, n):
            rep_sum = rep_sum + parts[d]
    else:
        rep_sum = lax.fori_loop(1, n, lambda d, c: c + parts[d], parts[0])
    rep = (rep_sum * (1.0 / (group * WIN))).astype(jnp.bfloat16)
    placed = jnp.dot(hits, rep, preferred_element_type=jnp.float32)
    bank[...] = jnp.where(taken > 0.5, placed, old.astype(jnp.float32)).astype(jnp.bfloat16)
    def drain(i):
        peer = lax.rem(me + 1 + i, n)
        key_copy(me, peer).wait_send()
        cache_copy(me, peer).wait_send()
        part_copy(me, peer, mine).wait_send()

    each(n - 1, drain)


def relate_kernel(q_v, bank, rel_hbm, bank_hbm, rel_v, sem):
    group, toks, dim = q_v.shape
    local = bank_hbm.shape[0]
    scale = 1.0 / math.sqrt(dim)
    first = pl.multiple_of(lax.axis_index("seq") * local, local)
    keep = pltpu.make_async_copy(bank.at[pl.ds(first, local)], bank_hbm, sem.at[group])
    keep.start()
    outs = [
        pltpu.make_async_copy(rel_v.at[j], rel_hbm.at[j], sem.at[j]) for j in range(group)
    ]
    for j in range(group):
        r = lax.dot_general(q_v[j], bank[...], NT, preferred_element_type=jnp.float32)
        rel_v[j] = (r * scale).astype(jnp.bfloat16)
        outs[j].start()
    for out in outs:
        out.wait()
    keep.wait()


def per_device(n, queries, new_keys, cache_keys, window_start, owner_slot):
    toks, group, dim = queries.shape
    ktoks, local = new_keys.shape[0], cache_keys.shape[0]
    blocks = window_start.shape[0]
    slots = n * local
    hbm_spec = pl.BlockSpec(memory_space=pltpu.HBM)
    vmem_spec = pl.BlockSpec(memory_space=pltpu.VMEM)
    bf16 = jnp.bfloat16
    q_held, bank = pl.pallas_call(
        functools.partial(refresh_kernel, n),
        out_shape=(
            pltpu.VMEM((group, toks, dim), bf16),
            pltpu.VMEM((slots, dim), bf16),
        ),
        in_specs=[hbm_spec] * 5,
        out_specs=(vmem_spec, vmem_spec),
        scratch_shapes=[
            pltpu.SMEM((blocks,), jnp.int32),
            pltpu.VMEM((1, blocks), jnp.int32),
            pltpu.VMEM((dim, group * toks), bf16),
            pltpu.VMEM((n, ktoks, dim), bf16),
            pltpu.VMEM((n, local, dim), bf16),
            pltpu.VMEM((blocks, dim), jnp.float32),
            pltpu.VMEM((n, blocks, dim), jnp.float32),
            pltpu.SemaphoreType.DMA((5,)),
        ] + [pltpu.SemaphoreType.DMA((n,))] * 6,
        compiler_params=pltpu.CompilerParams(
            collective_id=0, has_side_effects=True, vmem_limit_bytes=VMEM - 2 * dim * (group * toks + slots) - 16384
        ),
        name="refresh",
    )(
        window_start,
        owner_slot.reshape(1, blocks),
        jnp.transpose(queries, (1, 0, 2)),
        new_keys.reshape(ktoks, dim),
        cache_keys.reshape(local, dim),
    )
    rel, own = pl.pallas_call(
        relate_kernel,
        out_shape=(
            jax.ShapeDtypeStruct((group, toks, slots), bf16),
            jax.ShapeDtypeStruct((local, dim), bf16),
        ),
        in_specs=[vmem_spec, vmem_spec],
        out_specs=(hbm_spec, hbm_spec),
        scratch_shapes=[
            pltpu.VMEM((group, toks, slots), bf16),
            pltpu.SemaphoreType.DMA((group + 1,)),
        ],
        compiler_params=pltpu.CompilerParams(
            vmem_limit_bytes=2 * group * toks * slots + 16 * 1024 * 1024
        ),
        name="relate",
    )(q_held, bank)
    return jnp.transpose(rel, (1, 0, 2)), own[:, None, :]


def solution(mesh):
    spec = P("seq", "kvh", None)
    return jax.shard_map(
        functools.partial(per_device, mesh.shape["seq"]),
        mesh=mesh,
        in_specs=(spec, spec, spec, P(), P()),
        out_specs=(spec, spec),
        check_vma=False,
    )
```

```python
import functools
import math

import jax
import jax.numpy as jnp
from jax import lax
from jax.experimental import pallas as pl
from jax.experimental.pallas import tpu as pltpu
from jax.sharding import PartitionSpec as P

BLK = 128
WIN = 512
VMEM = 67043328
LOG2E = 1.4426950408889634
NT = (((1,), (1,)), ((), ()))


def each(count, body):
    if count <= 8:
        for i in range(count):
            body(i)
    else:
        lax.fori_loop(0, count, lambda i, c: (body(i), c)[1], 0)


def refresh_kernel(
    n, start_hbm, slot_hbm, q_hbm, k_hbm, c_hbm, q_v, bank,
    start_ref, slot_ref, q_t, keys, cache, mine, parts,
    load_sem, ks_sem, kr_sem, cs_sem, cr_sem, ps_sem, pr_sem,
):
    group, toks, dim = q_v.shape
    ktoks = keys.shape[1]
    local = cache.shape[1]
    slots = n * local
    per = ktoks // BLK
    blocks = n * per
    rows = group * toks
    scale = 1.0 / math.sqrt(dim)
    me = lax.axis_index("seq")

    load_k = pltpu.make_async_copy(k_hbm, keys.at[me], load_sem.at[0])
    load_q = pltpu.make_async_copy(q_hbm, q_v, load_sem.at[1])
    load_c = pltpu.make_async_copy(c_hbm, cache.at[me], load_sem.at[2])
    load_w = pltpu.make_async_copy(start_hbm, start_ref, load_sem.at[3])
    load_s = pltpu.make_async_copy(slot_hbm, slot_ref, load_sem.at[4])
    load_k.start()
    load_c.start()
    load_q.start()
    load_w.start()
    load_s.start()

    barrier = pltpu.get_barrier_semaphore()

    def greet(i):
        peer = lax.rem(me + 1 + i, n)
        pl.semaphore_signal(
            barrier, inc=1, device_id={"seq": peer}, device_id_type=pl.DeviceIdType.MESH
        )

    each(n - 1, greet)

    def link(src, dst, s_sem, r_sem, peer):
        return pltpu.make_async_remote_copy(
            src_ref=src, dst_ref=dst, send_sem=s_sem, recv_sem=r_sem,
            device_id={"seq": peer}, device_id_type=pl.DeviceIdType.MESH,
        )

    def key_copy(slot, peer):
        return link(keys.at[slot], keys.at[slot], ks_sem.at[peer], kr_sem.at[slot], peer)

    def cache_copy(slot, peer):
        return link(cache.at[slot], cache.at[slot], cs_sem.at[peer], cr_sem.at[slot], peer)

    def part_copy(slot, peer, src):
        return link(src, parts.at[slot], ps_sem.at[peer], pr_sem.at[slot], peer)

    load_q.wait()
    load_w.wait()
    load_s.wait()
    for j in range(group):
        q_t[:, j * toks:(j + 1) * toks] = q_v[j].T

    load_k.wait()
    position = me * toks + lax.broadcasted_iota(jnp.int32, (1, toks), 1)

    def partial(owner):
        for p in range(per):
            index = owner * per + p
            kb = keys[owner, p * BLK:(p + 1) * BLK, :]
            begin = start_ref[index]
            mask = jnp.where((position >= begin) & (position < begin + WIN), 1.0, 0.0)
            s = jnp.dot(kb, q_t[...], preferred_element_type=jnp.float32)
            top = jnp.max(s, axis=0, keepdims=True)
            e = jnp.exp2((s - top) * (scale * LOG2E))
            total = jnp.sum(e, axis=0, keepdims=True)
            acc = None
            for j in range(group):
                cols = slice(j * toks, (j + 1) * toks)
                term = e[:, cols] * (mask / total[:, cols])
                acc = term if acc is None else acc + term
            weight = jnp.sum(acc, axis=1, keepdims=True)
            rep = jnp.sum(weight * kb.astype(jnp.float32), axis=0, keepdims=True)
            mine[pl.ds(index, 1), :] = rep

    partial(me)

    pl.semaphore_wait(barrier, n - 1)
    each(n - 1, lambda i: key_copy(me, lax.rem(me + 1 + i, n)).start())
    load_c.wait()

    def arrive(i):
        owner = lax.rem(me + n - 1 - i, n)
        key_copy(owner, owner).wait_recv()
        partial(owner)

    each(n - 1, arrive)
    each(n - 1, lambda i: part_copy(me, lax.rem(me + 1 + i, n), mine).start())
    each(n - 1, lambda i: cache_copy(me, lax.rem(me + 1 + i, n)).start())

    each(n - 1, lambda i: cache_copy(lax.rem(me + n - 1 - i, n), me).wait_recv())
    hits = jnp.where(
        lax.broadcasted_iota(jnp.int32, (slots, blocks), 0) == slot_ref[...], 1.0, 0.0
    )
    taken = jnp.max(hits, axis=1, keepdims=True)
    hits = hits.astype(jnp.bfloat16)
    old = cache[...].reshape(slots, dim)

    each(n - 1, lambda i: part_copy(lax.rem(me + n - 1 - i, n), me, mine).wait_recv())
    parts[me] = mine[...]
    if n <= 8:
        rep_sum = parts[0]
        for d in range(1, n):
            rep_sum = rep_sum + parts[d]
    else:
        rep_sum = lax.fori_loop(1, n, lambda d, c: c + parts[d], parts[0])
    rep = (rep_sum * (1.0 / (group * WIN))).astype(jnp.bfloat16)
    placed = jnp.dot(hits, rep, preferred_element_type=jnp.float32)
    bank[...] = jnp.where(taken > 0.5, placed, old.astype(jnp.float32)).astype(jnp.bfloat16)
    def drain(i):
        peer = lax.rem(me + 1 + i, n)
        key_copy(me, peer).wait_send()
        cache_copy(me, peer).wait_send()
        part_copy(me, peer, mine).wait_send()

    each(n - 1, drain)


def relate_kernel(q_v, bank, rel_hbm, bank_hbm, rel_v, sem):
    group, toks, dim = q_v.shape
    local = bank_hbm.shape[0]
    scale = 1.0 / math.sqrt(dim)
    first = pl.multiple_of(lax.axis_index("seq") * local, local)
    keep = pltpu.make_async_copy(bank.at[pl.ds(first, local)], bank_hbm, sem.at[group])
    keep.start()
    outs = [
        pltpu.make_async_copy(rel_v.at[j], rel_hbm.at[j], sem.at[j]) for j in range(group)
    ]
    for j in range(group):
        r = lax.dot_general(q_v[j], bank[...], NT, preferred_element_type=jnp.float32)
        rel_v[j] = (r * scale).astype(jnp.bfloat16)
        outs[j].start()
    for out in outs:
        out.wait()
    keep.wait()


def per_device(n, queries, new_keys, cache_keys, window_start, owner_slot):
    toks, group, dim = queries.shape
    ktoks, local = new_keys.shape[0], cache_keys.shape[0]
    blocks = window_start.shape[0]
    slots = n * local
    hbm_spec = pl.BlockSpec(memory_space=pltpu.HBM)
    vmem_spec = pl.BlockSpec(memory_space=pltpu.VMEM)
    bf16 = jnp.bfloat16
    q_held, bank = pl.pallas_call(
        functools.partial(refresh_kernel, n),
        out_shape=(
            pltpu.VMEM((group, toks, dim), bf16),
            pltpu.VMEM((slots, dim), bf16),
        ),
        in_specs=[hbm_spec] * 5,
        out_specs=(vmem_spec, vmem_spec),
        scratch_shapes=[
            pltpu.SMEM((blocks,), jnp.int32),
            pltpu.VMEM((1, blocks), jnp.int32),
            pltpu.VMEM((dim, group * toks), bf16),
            pltpu.VMEM((n, ktoks, dim), bf16),
            pltpu.VMEM((n, local, dim), bf16),
            pltpu.VMEM((blocks, dim), jnp.float32),
            pltpu.VMEM((n, blocks, dim), jnp.float32),
            pltpu.SemaphoreType.DMA((5,)),
        ] + [pltpu.SemaphoreType.DMA((n,))] * 6,
        compiler_params=pltpu.CompilerParams(
            collective_id=0, has_side_effects=True, vmem_limit_bytes=VMEM - 2 * dim * (group * toks + slots) - 16384
        ),
        name="refresh",
    )(
        window_start,
        owner_slot.reshape(1, blocks),
        jnp.transpose(queries, (1, 0, 2)),
        new_keys.reshape(ktoks, dim),
        cache_keys.reshape(local, dim),
    )
    rel, own = pl.pallas_call(
        relate_kernel,
        out_shape=(
            jax.ShapeDtypeStruct((group, toks, slots), bf16),
            jax.ShapeDtypeStruct((local, dim), bf16),
        ),
        in_specs=[vmem_spec, vmem_spec],
        out_specs=(hbm_spec, hbm_spec),
        scratch_shapes=[
            pltpu.VMEM((group, toks, slots), bf16),
            pltpu.SemaphoreType.DMA((group + 1,)),
        ],
        compiler_params=pltpu.CompilerParams(
            vmem_limit_bytes=2 * group * toks * slots + 16 * 1024 * 1024
        ),
        name="relate",
    )(q_held, bank)
    return jnp.transpose(rel, (1, 0, 2)), own[:, None, :]


def solution(mesh):
    spec = P("seq", "kvh", None)
    return jax.shard_map(
        functools.partial(per_device, mesh.shape["seq"]),
        mesh=mesh,
        in_specs=(spec, spec, spec, P(), P()),
        out_specs=(spec, spec),
        check_vma=False,
    )
```
